32 devices in a mesh: dp: 16 (over z, y, x), seq: 2 (over core).
Axes of the slice: x: 2, y: 2, z: 4, core: 2. Of those that a mesh axis runs over, the one named last changes fastest.
Arguments:
- patches: bfloat16 [32, 256, 768], P('dp', 'seq'), may hold values from -6 to 6
- block_masks: int32 [32, 196], P('dp'), may hold values from 0 to 1, as said below
- split_rows: int32 [32], P('dp'), may hold values from 6 to 8, as said below
- span_order: int32 [2720], replicated, may hold values from 0 to 2719, as said below
- weights: float32 [10880, 768], P('dp')
- teacher: bfloat16 [10880, 768], P('dp')
- first_moment: float32 [10880, 768], P('dp')
- second_moment: float32 [10880, 768], P('dp')
- step_count: int32 [1], replicated, may hold values from 2 to 20
Outputs:
- total_loss: float32 [], replicated
- grad_norm: float32 [], replicated
- updated_weights: float32 [10880, 768], P('dp')
- weights_copy: bfloat16 [10880, 768], P('dp')
- updated_first: float32 [10880, 768], P('dp')
- updated_second: float32 [10880, 768], P('dp')
The draws below stay inside these ranges and needn't reach their ends.
Inputs may be any that keep to these rules, and one draw needn't show every extreme that they name: `block_masks`: cells are row-major over the 14 x 14 grid; masks come in aligned 2 x 2 blocks of cells. Rows 0 to split_rows - 1 of an image lie on seq index 0 after its CLS slot, the rest on seq index 1 from slot 0. `span_order`: each of 0 to 2719 once.
All inputs are finite; a program needn't handle non-finite values.
Results may differ from the reference program's by a relative error of at most 0.001.
The reference program's roundings to bfloat16 on the way count: a program that leaves them out, or rounds other values in their place, can miss the bound.
Values may be sent and summed in bfloat16 or wider, within the bound.
A program may use at most 256 MiB of HBM per device.

```python
import math
import jax
import jax.numpy as jnp
import numpy as np
from jax import lax

D = 768
HEADS = 12
HD = 64
FF = 3072
PP = 768
GRID = 14
SL = 128
CR = 4
IMAGES = 32
PROWS = 10768
NCH = 2720
FLAT = 10880


CLIP = 0.01


def layout_drawn():
    return [('cls', 1, (D,)), ('mask_tok', 1, (D,)), ('b_pe', 1, (D,)), ('ln1_g', 1, (D,)), ('ln1_b', 1, (D,)), ('b_out', 1, (D,)), ('ln2_g', 1, (D,)), ('ln2_b', 1, (D,)), ('b_two', 1, (D,)), ('lnf_g', 1, (D,)), ('lnf_b', 1, (D,)), ('b_head', 1, (D,)), ('b_one', FF // D, (FF,)), ('w_pe', PP, (PP, D)), ('w_qkv', 3 * D, (D, 3 * D)), ('w_out', D, (D, D)), ('w_one', FF, (D, FF)), ('w_two', FF, (FF, D)), ('w_head', D, (D, D))]


def span_perm(key):
    return jax.random.permutation(jax.random.fold_in(key, 11), NCH).astype(jnp.int32)


def row_tables():
    centre = np.zeros(FLAT, np.float32)
    spread_rows = np.full(FLAT, 0.02, np.float32)
    grad_rows = np.full(FLAT, 1.0, np.float32)
    spreads = {'cls': 0.5, 'mask_tok': 0.5, 'b_pe': 0.2, 'ln1_g': 0.1, 'ln1_b': 0.1, 'b_out': 0.1, 'ln2_g': 0.1, 'ln2_b': 0.1, 'b_two': 0.1, 'lnf_g': 0.1, 'lnf_b': 0.1, 'b_head': 0.1, 'b_one': 0.1, 'w_pe': PP ** (-0.5), 'w_qkv': 1.5 * D ** (-0.5), 'w_out': 4.0 * D ** (-0.5), 'w_one': D ** (-0.5), 'w_two': FF ** (-0.5), 'w_head': D ** (-0.5)}
    offset = 0
    for entry_name, entry_rows, entry_shape in layout_drawn():
        spread_rows[offset:offset + entry_rows] = spreads[entry_name]
        if entry_name in ('ln1_g', 'ln2_g', 'lnf_g'):
            centre[offset:offset + entry_rows] = 1.0
        if len(entry_shape) == 1:
            grad_rows[offset:offset + entry_rows] = 4.0
        offset = offset + entry_rows
    return (centre, spread_rows, grad_rows)


def stored_layout(key, logical):
    return logical.reshape(NCH, CR, D)[span_perm(key)].reshape(FLAT, D)


def draw_span_order(key, part):
    return span_perm(key)


def draw_weights(key, part):
    centre, spread_rows, grad_rows = row_tables()
    subkey = jax.random.fold_in(key, 21)
    noise = jax.random.normal(subkey, (FLAT, D), jnp.float32)
    return stored_layout(key, jnp.asarray(centre)[:, None] + jnp.asarray(spread_rows)[:, None] * noise)


def draw_teacher(key, part):
    centre, spread_rows, grad_rows = row_tables()
    subkey = jax.random.fold_in(key, 22)
    noise = jax.random.normal(subkey, (FLAT, D), jnp.float32)
    logical = jnp.asarray(centre)[:, None] + jnp.asarray(spread_rows)[:, None] * noise
    return stored_layout(key, logical).astype(jnp.bfloat16)


def draw_first_moment(key, part):
    centre, spread_rows, grad_rows = row_tables()
    grad_scale = jnp.asarray(grad_rows)[:, None] * (CLIP / math.sqrt(PROWS * D))
    subkey = jax.random.fold_in(key, 23)
    noise = jax.random.normal(subkey, (FLAT, D), jnp.float32)
    return stored_layout(key, 0.11 * grad_scale * noise)


def draw_second_moment(key, part):
    centre, spread_rows, grad_rows = row_tables()
    grad_scale = jnp.asarray(grad_rows)[:, None] * (CLIP / math.sqrt(PROWS * D))
    subkey = jax.random.fold_in(key, 24)
    multiple = jnp.exp(jax.random.uniform(subkey, (FLAT, D), jnp.float32, 0.0, math.log(4.0)))
    return stored_layout(key, 0.001 * grad_scale * grad_scale * multiple)


def draw_block_masks(key, part):
    coarse = (jax.random.randint(jax.random.fold_in(key, 31), (IMAGES, GRID // 2, GRID // 2), 0, 5) < 3).astype(jnp.int32)
    upsampled = jnp.repeat(jnp.repeat(coarse, 2, 1), 2, 2)
    return upsampled.reshape(IMAGES, GRID * GRID)


def draw_split_rows(key, part):
    drawn = jax.random.randint(jax.random.fold_in(key, 41), (IMAGES,), GRID // 2 - 1, GRID // 2 + 2).astype(jnp.int32)
    return drawn.at[0].set(GRID // 2 + 1).at[1].set(GRID // 2 - 1)


def block_scale(stream_key, shape, cuts, low, high):
    factor_of = 1.0
    for dim, shards_of in cuts:
        heights = jax.random.uniform(jax.random.fold_in(jax.random.fold_in(stream_key, 6), dim), (shards_of,), jnp.float32, low / len(cuts), high / len(cuts))
        factor_of = factor_of * jnp.repeat(jnp.exp(heights), shape[dim] // shards_of).reshape((-1,) + (1,) * (len(shape) - 1 - dim))
    return factor_of


def gaussian(rng, dims, width, bound, split=(), kind=jnp.bfloat16):
    values = width * jax.random.normal(rng, dims, jnp.float32)
    if split:
        values = values * block_scale(rng, dims, split, -0.22, 0.18)
    return jnp.clip(values, -bound, bound).astype(kind)


def setup_inputs(seed: int = 0) -> dict:
    keys = jax.random.split(jax.random.key(seed), 10)
    return {
        "patches": gaussian(keys[0], (IMAGES, 2 * SL, PP), 1.0, 6.0, ((0, 16), (1, 2))),
        "block_masks": draw_block_masks(jax.random.fold_in(keys[9], 71), 0),
        "split_rows": draw_split_rows(jax.random.fold_in(keys[9], 71), 0),
        "span_order": draw_span_order(jax.random.fold_in(keys[9], 71), 0),
        "weights": draw_weights(jax.random.fold_in(keys[9], 71), 0),
        "teacher": draw_teacher(jax.random.fold_in(keys[9], 71), 0),
        "first_moment": draw_first_moment(jax.random.fold_in(keys[9], 71), 0),
        "second_moment": draw_second_moment(jax.random.fold_in(keys[9], 71), 0),
        "step_count": jax.random.randint(keys[8], (1,), 2, 21).astype(jnp.int32),
    }


@jax.custom_vjp
def low(v):
    return lax.optimization_barrier(v.astype(jnp.bfloat16)).astype(jnp.float32)

@jax.custom_vjp
def low_back(v):
    return v

def low_keep(v):
    return (low(v), None)

def low_pass(kept, grad):
    return (grad,)

def back_keep(v):
    return (v, None)

def back_low(kept, grad):
    return (low(grad),)
low.defvjp(low_keep, low_pass)
low_back.defvjp(back_keep, back_low)
HIGHEST = lax.Precision.HIGHEST
BETA = 2.0
CLIP = 0.01
LEARN = 0.03
DECAY = 0.05
BETA_ONE = 0.9
BETA_TWO = 0.999
ADAM_EPS = 1e-08
NORM_EPS = 1e-06

def layout():
    return [('cls', 1, (D,)), ('mask_tok', 1, (D,)), ('b_pe', 1, (D,)), ('ln1_g', 1, (D,)), ('ln1_b', 1, (D,)), ('b_out', 1, (D,)), ('ln2_g', 1, (D,)), ('ln2_b', 1, (D,)), ('b_two', 1, (D,)), ('lnf_g', 1, (D,)), ('lnf_b', 1, (D,)), ('b_head', 1, (D,)), ('b_one', FF // D, (FF,)), ('w_pe', PP, (PP, D)), ('w_qkv', 3 * D, (D, 3 * D)), ('w_out', D, (D, D)), ('w_one', FF, (D, FF)), ('w_two', FF, (FF, D)), ('w_head', D, (D, D))]

def unpack(flat):
    tables = {}
    offset = 0
    for entry_name, entry_rows, entry_shape in layout():
        tables[entry_name] = flat[offset:offset + entry_rows].reshape(entry_shape)
        offset = offset + entry_rows
    return tables

def pack_flat(tables, total_rows):
    pieces = [tables[entry_name].reshape(-1, D) for entry_name, entry_rows, entry_shape in layout()]
    stacked = jnp.concatenate(pieces, 0)
    return jnp.concatenate([stacked, jnp.zeros((total_rows - stacked.shape[0], D), stacked.dtype)], 0)

def reorder(stored, order):
    return stored.reshape(order.shape[0], -1, D)[order].reshape(-1, D)

def slot_info(split_rows, seq_side):
    column = jnp.arange(SL)[None, :]
    split_col = split_rows[:, None]
    first_side = seq_side == 0
    first_slot = jnp.where(first_side, 1, 0)
    filled = jnp.where(first_side, split_col * GRID, (GRID - split_col) * GRID)
    offset = jnp.where(first_side, -1, split_col * GRID)
    is_patch = (column >= first_slot) & (column < first_slot + filled)
    is_cls = first_side & (column == 0) & (split_col >= 0)
    grid_cell = jnp.clip(column + offset, 0, GRID * GRID - 1).astype(jnp.int32)
    return (is_patch, is_cls, grid_cell)

def sincos(grid_cell):
    quarter = D // 4
    frequency = 1.0 / 10000.0 ** (jnp.arange(quarter).astype(jnp.float32) / quarter)
    rows_at = (grid_cell // GRID).astype(jnp.float32)[..., None] * frequency
    cols_at = (grid_cell % GRID).astype(jnp.float32)[..., None] * frequency
    return jnp.concatenate([jnp.sin(rows_at), jnp.cos(rows_at), jnp.sin(cols_at), jnp.cos(cols_at)], -1)

def layer_norm(values):
    center = lax.optimization_barrier(jnp.mean(values, -1, keepdims=True))
    centred = values - center
    return centred * lax.rsqrt(lax.optimization_barrier(jnp.mean(centred * centred, -1, keepdims=True)) + NORM_EPS)

def embed_tokens(params, pixels, is_patch, is_cls, hidden_mask, position):
    embedded = low_back(jnp.dot(pixels, params['w_pe'], precision=HIGHEST) + params['b_pe'])
    tokens = jnp.where(is_patch[..., None], embedded + position, 0.0)
    tokens = jnp.where(hidden_mask[..., None], params['mask_tok'] + position, tokens)
    return jnp.where(is_cls[..., None], params['cls'], tokens)

def block_forward(params, tokens, key_live):
    groups, length = (tokens.shape[0], tokens.shape[1])
    normed = low(layer_norm(tokens) * params['ln1_g'] + params['ln1_b'])
    packed = low_back(low(jnp.dot(normed, params['w_qkv'], precision=HIGHEST))).reshape(groups, length, 3, HEADS, HD)
    queries, keys_all, values_all = (packed[:, :, 0], packed[:, :, 1], packed[:, :, 2])
    scores = low_back(jnp.einsum('gqhd,gkhd->ghqk', queries, keys_all, precision=HIGHEST) * HD ** (-0.5))
    scores = jnp.where(key_live[:, None, None, :], scores, -1e+30)
    exponent = jnp.exp(scores - lax.optimization_barrier(jnp.max(scores, -1, keepdims=True)))
    attention = exponent / lax.optimization_barrier(jnp.sum(exponent, -1, keepdims=True))
    mixed_out = jnp.einsum('ghqk,gkhd->gqhd', low(attention), values_all, precision=HIGHEST)
    mixed_out = low_back(low(mixed_out)).reshape(groups, length, D)
    hidden = tokens + low_back(jnp.dot(mixed_out, params['w_out'], precision=HIGHEST) + params['b_out'])
    normed_two = low(layer_norm(hidden) * params['ln2_g'] + params['ln2_b'])
    upward = low_back(jnp.dot(normed_two, params['w_one'], precision=HIGHEST) + params['b_one'])
    gelled = low(jax.nn.gelu(upward))
    return hidden + low_back(jnp.dot(gelled, params['w_two'], precision=HIGHEST) + params['b_two'])

def reference(patches, block_masks, split_rows, span_order, weights, teacher, first_moment, second_moment, step_count):
    inverse_order = jnp.argsort(span_order).astype(jnp.int32)
    student = unpack(reorder(weights, inverse_order).astype(jnp.bfloat16).astype(jnp.float32))
    teacher_params = unpack(reorder(teacher, inverse_order).astype(jnp.float32))
    patch_zero, cls_zero, cell_zero = slot_info(split_rows, 0)
    patch_one, cls_one, cell_one = slot_info(split_rows, 1)
    is_patch = jnp.concatenate([patch_zero, patch_one], 1)
    is_cls = jnp.concatenate([cls_zero, cls_one], 1)
    grid_cell = jnp.concatenate([cell_zero, cell_one], 1)
    hidden_mask = (jnp.take_along_axis(block_masks, grid_cell, 1) == 1) & is_patch
    masked_count = jnp.sum(hidden_mask.astype(jnp.float32))
    loss_scale = 1.0 / (math.sqrt(D) * masked_count)
    position = sincos(grid_cell)
    batches = IMAGES // 16

    def split_groups(values):
        return values.reshape((batches, 16) + values.shape[1:])
    stacked_inputs = tuple((split_groups(member) for member in (patches, hidden_mask, is_patch, is_cls, position)))

    def group_step(carried, group):
        pixel_group, mask_group, patch_group, cls_group, position_group = group
        key_live = patch_group | cls_group
        pixels = pixel_group.astype(jnp.float32)
        teacher_tokens = embed_tokens(teacher_params, pixels, patch_group, cls_group, jnp.zeros_like(mask_group), position_group)
        target = layer_norm(block_forward(teacher_params, teacher_tokens, key_live))

        def loss_of(params):
            tokens = embed_tokens(params, pixels, patch_group, cls_group, mask_group, position_group)
            output = block_forward(params, tokens, key_live)
            final = low(layer_norm(output) * params['lnf_g'] + params['lnf_b'])
            predicted = low_back(jnp.dot(final, params['w_head'], precision=HIGHEST) + params['b_head'])
            difference = predicted - target
            magnitude = jnp.abs(difference)
            elementwise = jnp.where(magnitude < BETA, 0.5 * difference * difference / BETA, magnitude - 0.5 * BETA)
            return jnp.sum(jnp.where(mask_group[..., None], elementwise, 0.0)) * loss_scale
        loss_value, loss_pull = jax.vjp(loss_of, student)
        gradients, = loss_pull(jnp.ones_like(loss_value))
        return ((carried[0] + loss_value, jax.tree.map(jnp.add, carried[1], gradients)), None)
    zeros_tree = jax.tree.map(jnp.zeros_like, student)
    (total_loss, gradients), unused = lax.scan(group_step, (jnp.zeros((), jnp.float32), zeros_tree), stacked_inputs)
    stored_grad = reorder(pack_flat(gradients, weights.shape[0]), span_order)
    grad_norm = jnp.sqrt(jnp.sum(stored_grad * stored_grad))
    clipped = stored_grad * (CLIP / jnp.maximum(grad_norm, CLIP))
    updated_first = BETA_ONE * first_moment + (1.0 - BETA_ONE) * clipped
    updated_second = BETA_TWO * second_moment + (1.0 - BETA_TWO) * clipped * clipped
    steps_done = step_count[0].astype(jnp.float32)
    adam_step = updated_first / (1.0 - BETA_ONE ** steps_done) / (jnp.sqrt(updated_second / (1.0 - BETA_TWO ** steps_done)) + ADAM_EPS)
    updated_weights = weights - LEARN * (adam_step + DECAY * weights)
    return (total_loss, grad_norm, updated_weights, updated_weights.astype(jnp.bfloat16), updated_first, updated_second)
```

```python
import functools
import math

import jax
import jax.numpy as jnp
from jax import lax
from jax.experimental import pallas as pl
from jax.experimental.pallas import tpu as pltpu
from jax.sharding import PartitionSpec as P

D = 768
HEADS = 12
HD = 64
FF = 3072
PP = 768
GRID = 14
SL = 128
CR = 4


BETA = 2.0
CLIP = 0.01
LEARN = 0.03
DECAY = 0.05
BETA_ONE = 0.9
BETA_TWO = 0.999
ADAM_EPS = 1e-08
NORM_EPS = 1e-06


def from_partner(shard, axis, bit):
    return lax.ppermute(shard, axis, [(i, i ^ 1 << bit) for i in range(lax.axis_size(axis))])


MESH = pl.DeviceIdType.MESH
ZN = 4


def place():
    p = lax.axis_index("dp")
    return p, p // 4, (p // 2) % 2, p % 2, lax.axis_index("seq")


def to_chip(p, s):
    return (p, s)


def greet(p, z, s):
    barrier = pltpu.get_barrier_semaphore()

    def hello(dev):
        pl.semaphore_signal(barrier, inc=1, device_id=dev, device_id_type=MESH)

    hello((p, 1 - s))
    hello((p ^ 1, s))
    hello((p ^ 2, s))

    @pl.when(z > 0)
    def _():
        hello((p - 4, s))

    @pl.when(z < ZN - 1)
    def _():
        hello((p + 4, s))

    ends = jnp.where(z == 0, 1, 0) + jnp.where(z == ZN - 1, 1, 0)
    pl.semaphore_wait(barrier, 5 - ends)


def gather_kernel(nq, nk, *refs):
    src = refs[:nq]
    out = refs[nq : 2 * nq]
    send_sem, recv_sem, psend_sem, precv_sem, own_sem = refs[2 * nq :]
    p, z, y, x, s = place()

    def span(q, k, side):
        half = src[q].shape[0] // 2
        low, high = half * k // nk, half * (k + 1) // nk
        return pl.ds(side * half + low, high - low)

    def rows(q, k):
        return span(q, k, s)

    def far_rows(q, k):
        return span(q, k, 1 - s)

    def dest(way):
        if way == "u":
            return p + 4
        if way == "d":
            return p - 4
        return p ^ 1 if way == "x" else p ^ 2

    LANE = {"u": 0, "d": 1, "x": 2, "y": 3}

    def copy(q, k, origin, way, own):
        block = src[q].at[rows(q, k)] if own else out[q].at[origin, rows(q, k)]
        return pltpu.make_async_remote_copy(
            src_ref=block,
            dst_ref=out[q].at[origin, rows(q, k)],
            send_sem=send_sem.at[LANE[way], q, k, origin],
            recv_sem=recv_sem.at[q, k, origin],
            device_id=(dest(way), s),
            device_id_type=MESH,
        )

    def arrive(q, k, origin):
        pltpu.make_async_remote_copy(
            src_ref=out[q].at[origin, rows(q, k)],
            dst_ref=out[q].at[origin, rows(q, k)],
            send_sem=send_sem.at[0, q, k, origin],
            recv_sem=recv_sem.at[q, k, origin],
            device_id=(p, s),
            device_id_type=MESH,
        ).wait_recv()

    def hand(q, k, origin):
        return pltpu.make_async_remote_copy(
            src_ref=out[q].at[origin, rows(q, k)],
            dst_ref=out[q].at[origin, rows(q, k)],
            send_sem=psend_sem.at[q, k, origin],
            recv_sem=precv_sem.at[q, k, origin],
            device_id=(p, 1 - s),
            device_id_type=MESH,
        )

    greet(p, z, s)
    pieces = [(q, k) for q in range(nq) for k in range(nk)]
    first = lambda k: "x" if k % 2 == 0 else "y"
    second = lambda k: "y" if k % 2 == 0 else "x"
    log = []

    def go(cond, fn):
        if cond is None:
            fn()
        else:
            pl.when(cond)(fn)

    def start(cond, c):
        go(cond, c.start)
        log.append((cond, c.wait_send))

    def both(a, b):
        return b if a is None else a & b

    for q, k in pieces:
        start(z < ZN - 1, copy(q, k, p, "u", True))
        start(z > 0, copy(q, k, p, "d", True))
        start(None, copy(q, k, p, first(k), True))
        start(None, copy(q, k, p, second(k), True))
    owned = [pltpu.make_async_copy(src[q], out[q].at[p], own_sem.at[q]) for q in range(nq)]
    for c in owned:
        c.start()

    offsets = [0]
    for d in range(1, ZN):
        offsets += [-d, d]
    for q in range(nq):
        for d in offsets:
            ok = None if d == 0 else ((z + d >= 0) & (z + d < ZN))
            o = p + 4 * d
            for k in range(nk):
                if d != 0:
                    def relay(k=k, o=o, d=d):
                        arrive(q, k, o)

                    go(ok, relay)
                    if d < 0:
                        start(both(ok, z < ZN - 1), copy(q, k, o, "u", False))
                    else:
                        start(both(ok, z > 0), copy(q, k, o, "d", False))
                    start(ok, copy(q, k, o, first(k), False))
                    start(ok, copy(q, k, o, second(k), False))
                    start(ok, hand(q, k, o))
            for k in range(nk):
                o1 = (p ^ (1 if first(k) == "x" else 2)) + 4 * d
                go(ok, lambda: arrive(q, k, o1))
                start(ok, copy(q, k, o1, second(k), False))
                start(ok, hand(q, k, o1))
            for k in range(nk):
                o2 = (p ^ (2 if first(k) == "x" else 1)) + 4 * d
                go(ok, lambda: arrive(q, k, o2))
                start(ok, hand(q, k, o2))
            for k in range(nk):
                o3 = (p ^ 3) + 4 * d
                go(ok, lambda: arrive(q, k, o3))
                start(ok, hand(q, k, o3))
    for c in owned:
        c.wait()
    for cond, w in log:
        go(cond, w)
    for q in range(nq):
        for k in range(nk):
            for flip in range(4):
                for d in offsets:
                    if d == 0 and flip == 0:
                        continue
                    ok = None if d == 0 else ((z + d >= 0) & (z + d < ZN))
                    o = (p ^ flip) + 4 * d

                    def take(q=q, k=k, o=o):
                        pltpu.make_async_remote_copy(
                            src_ref=out[q].at[o, far_rows(q, k)],
                            dst_ref=out[q].at[o, far_rows(q, k)],
                            send_sem=psend_sem.at[q, k, o],
                            recv_sem=precv_sem.at[q, k, o],
                            device_id=(p, 1 - s),
                            device_id_type=MESH,
                        ).wait_recv()

                    go(ok, take)


def gather_all(shards, dp, cid, nk=2):
    nq = len(shards)
    shapes = [jax.ShapeDtypeStruct((dp,) + shard.shape, shard.dtype) for shard in shards]
    return pl.pallas_call(
        functools.partial(gather_kernel, nq, nk),
        out_shape=shapes,
        in_specs=[pl.BlockSpec(memory_space=pltpu.VMEM)] * nq,
        out_specs=[pl.BlockSpec(memory_space=pl.ANY)] * nq,
        scratch_shapes=[
            pltpu.SemaphoreType.DMA((4, nq, nk, dp)),
            pltpu.SemaphoreType.DMA((nq, nk, dp)),
            pltpu.SemaphoreType.DMA((nq, nk, dp)),
            pltpu.SemaphoreType.DMA((nq, nk, dp)),
            pltpu.SemaphoreType.DMA((nq,)),
        ],
        compiler_params=pltpu.CompilerParams(
            collective_id=cid, has_side_effects=True, vmem_limit_bytes=60 * 2**20
        ),
        name="gather_all",
    )(*shards)


def scatter_kernel(cuts, g_ref, note_ref, out_ref, tot_ref, acc, pr, r1, r2, ru, rd,
                   sbuf, rbuf, zbuf, loc_sem, pair_s, pair_r, d1_s, d1_r, d2_s, d2_r,
                   up_s, up_r, dn_s, dn_r, fin_s, fin_r, sc_s, sc_r, zu_s, zu_r, zd_s, zd_r):
    p, z, y, x, s = place()
    H = cuts[-1]
    over = 2 * H - out_ref.shape[0]
    base = s * (H - over)
    far = (1 - s) * (H - over)
    nk = len(cuts) - 1

    def rows(k, first=0):
        return pl.ds(first + cuts[k], cuts[k + 1] - cuts[k])

    def remote(src, dst, a, b, dev):
        return pltpu.make_async_remote_copy(src_ref=src, dst_ref=dst, send_sem=a, recv_sem=b,
                                            device_id=dev, device_id_type=MESH)

    def load(k):
        return pltpu.make_async_copy(g_ref.at[:, :, :, rows(k, base)],
                                     acc.at[:, :, :, rows(k)], loc_sem.at[k])

    def pair(k):
        return remote(g_ref.at[:, :, :, rows(k, far)], pr.at[:, :, :, rows(k)],
                      pair_s.at[k], pair_r.at[k], (p, 1 - s))

    def one(k):
        if k % 2 == 0:
            src, dst, dev = acc.at[:, :, 1 - x, rows(k)], r1.at[:, :, rows(k)], (p ^ 1, s)
        else:
            src, dst, dev = acc.at[:, 1 - y, :, rows(k)], r1.at[:, :, rows(k)], (p ^ 2, s)
        return remote(src, dst, d1_s.at[k], d1_r.at[k], dev)

    def two(k):
        if k % 2 == 0:
            src, dev = acc.at[:, 1 - y, x, rows(k)], (p ^ 2, s)
        else:
            src, dev = acc.at[:, y, 1 - x, rows(k)], (p ^ 1, s)
        return remote(src, r2.at[:, rows(k)], d2_s.at[k], d2_r.at[k], dev)

    def up(k, t):
        return remote(acc.at[t, y, x, rows(k)], ru.at[t, rows(k)], up_s.at[k, t], up_r.at[k, t],
                      (p + 4, s))

    def down(k, t):
        return remote(acc.at[t, y, x, rows(k)], rd.at[t, rows(k)], dn_s.at[k, t], dn_r.at[k, t],
                      (p - 4, s))

    def add_up(k, t):
        acc[t, y, x, rows(k)] += ru[t, rows(k)]

    def add_down(k, t):
        acc[t, y, x, rows(k)] += rd[t, rows(k)]

    greet(p, z, s)
    for k in range(nk):
        pair(k).start()
        load(k).start()

    def stage_pair(k):
        load(k).wait()
        pair(k).wait_recv()

        def body(i, c):
            a, b, d = i // 4, (i // 2) % 2, i % 2
            acc[a, b, d, rows(k)] += pr[a, b, d, rows(k)]
            return c

        lax.fori_loop(0, 16, body, 0)
        one(k).start()

    def stage_one(k):
        one(k).wait_recv()

        def body(i, c):
            a, b = i // 2, i % 2
            if k % 2 == 0:
                acc[a, b, x, rows(k)] += r1[a, b, rows(k)]
            else:
                acc[a, y, b, rows(k)] += r1[a, b, rows(k)]
            return c

        lax.fori_loop(0, 8, body, 0)
        two(k).start()

    def stage_two(k):
        two(k).wait_recv()

        def body(a, c):
            acc[a, y, x, rows(k)] += r2[a, rows(k)]
            return c

        lax.fori_loop(0, 4, body, 0)

        @pl.when(z == 0)
        def _():
            for t in range(ZN - 1, 0, -1):
                up(k, t).start()

        @pl.when(z == ZN - 1)
        def _():
            for t in range(ZN - 1):
                down(k, t).start()

    def stage_z(k, i):
        t = ZN - 1 - i

        @pl.when((z > 0) & (z < t))
        def _():
            up(k, t).wait_recv()
            add_up(k, t)
            up(k, t).start()

        @pl.when((z < ZN - 1) & (z > i))
        def _():
            down(k, i).wait_recv()
            add_down(k, i)
            down(k, i).start()

    def stage_last(k):
        @pl.when(z > 0)
        def _():
            up(k, z).wait_recv()
            add_up(k, z)

        @pl.when(z < ZN - 1)
        def _():
            down(k, z).wait_recv()
            add_down(k, z)

    stages = [stage_pair, stage_one, stage_two] + [
        functools.partial(lambda i, k: stage_z(k, i), i) for i in range(ZN - 1)
    ] + [stage_last]
    for t in range(nk + len(stages) - 1):
        for j in range(len(stages)):
            if 0 <= t - j < nk:
                stages[j](t - j)

    low = lambda: remote(acc.at[z, y, x, pl.ds(0, H)], out_ref.at[pl.ds(0, H)],
                         fin_s, fin_r, (p, 1 - s))
    high = lambda: remote(acc.at[z, y, x, pl.ds(over, H - over)],
                          out_ref.at[pl.ds(H, H - over)], fin_s, fin_r, (p, 1 - s))

    @pl.when(s == 0)
    def _():
        low().start()
        out_ref[pl.ds(0, H)] = acc[z, y, x, pl.ds(0, H)]

    @pl.when(s == 1)
    def _():
        high().start()
        out_ref[pl.ds(H, H - over)] = acc[z, y, x, pl.ds(over, H - over)]

    mine = acc[z, y, x, pl.ds(over, H - over)]
    sq = jnp.sum(mine * mine)
    for i in range(over):
        head = acc[z, y, x, i]
        sq = sq + jnp.where(s == 0, jnp.sum(head * head), 0.0)
    row = lax.broadcasted_iota(jnp.int32, (8, 128), 0)
    cur = jnp.where(row == 1, sq, note_ref[...])
    for j, dev in enumerate([(p, 1 - s), (p ^ 1, s), (p ^ 2, s)]):
        sbuf[j] = cur
        c = remote(sbuf.at[j], rbuf.at[j], sc_s.at[j], sc_r.at[j], dev)
        c.start()
        c.wait()
        cur = cur + rbuf[j]
    zbuf[z] = cur

    def zup(o):
        return remote(zbuf.at[o], zbuf.at[o], zu_s.at[o], zu_r.at[o], (p + 4, s))

    def zdn(o):
        return remote(zbuf.at[o], zbuf.at[o], zd_s.at[o], zd_r.at[o], (p - 4, s))

    @pl.when(z < ZN - 1)
    def _():
        zup(z).start()

    @pl.when(z > 0)
    def _():
        zdn(z).start()

    for d in range(1, ZN):
        @pl.when(z - d >= 0)
        def _():
            zup(z - d).wait_recv()

        @pl.when((z - d >= 0) & (z < ZN - 1))
        def _():
            zup(z - d).start()

        @pl.when(z + d < ZN)
        def _():
            zdn(z + d).wait_recv()

        @pl.when((z + d < ZN) & (z > 0))
        def _():
            zdn(z + d).start()

    total = zbuf[0]
    for i in range(1, ZN):
        total = total + zbuf[i]
    tot_ref[...] = total

    @pl.when(s == 0)
    def _():
        low().wait_send()
        high().wait_recv()

    @pl.when(s == 1)
    def _():
        high().wait_send()
        low().wait_recv()

    for k in range(nk):
        pair(k).wait_send()
        one(k).wait_send()
        two(k).wait_send()
        for t in range(ZN):
            @pl.when(z < t)
            def _():
                up(k, t).wait_send()

            @pl.when(z > t)
            def _():
                down(k, t).wait_send()
    for o in range(ZN):
        @pl.when((o <= z) & (z < ZN - 1))
        def _():
            zup(o).wait_send()

        @pl.when((o >= z) & (z > 0))
        def _():
            zdn(o).wait_send()


def scatter_all(grads, note, cid, nk=6):
    dp, tiles = grads.shape[0], grads.shape[1]
    H = (tiles + 1) // 2
    cuts = [H * i // nk for i in range(nk + 1)]
    dma = pltpu.SemaphoreType.DMA
    box = (8, D)
    return pl.pallas_call(
        functools.partial(scatter_kernel, cuts),
        out_shape=[
            jax.ShapeDtypeStruct((tiles,) + box, jnp.float32),
            jax.ShapeDtypeStruct((8, 128), jnp.float32),
        ],
        in_specs=[pl.BlockSpec(memory_space=pl.ANY), pl.BlockSpec(memory_space=pltpu.VMEM)],
        out_specs=[pl.BlockSpec(memory_space=pltpu.VMEM)] * 2,
        scratch_shapes=[
            pltpu.VMEM((ZN, 2, 2, H) + box, jnp.float32),
            pltpu.VMEM((ZN, 2, 2, H) + box, jnp.float32),
            pltpu.VMEM((ZN, 2, H) + box, jnp.float32),
            pltpu.VMEM((ZN, H) + box, jnp.float32),
            pltpu.VMEM((ZN, H) + box, jnp.float32),
            pltpu.VMEM((ZN, H) + box, jnp.float32),
            pltpu.VMEM((3, 8, 128), jnp.float32),
            pltpu.VMEM((3, 8, 128), jnp.float32),
            pltpu.VMEM((ZN, 8, 128), jnp.float32),
            dma((nk,)), dma((nk,)), dma((nk,)), dma((nk,)), dma((nk,)), dma((nk,)), dma((nk,)),
            dma((nk, ZN)), dma((nk, ZN)), dma((nk, ZN)), dma((nk, ZN)),
            dma, dma, dma((3,)), dma((3,)), dma((ZN,)), dma((ZN,)), dma((ZN,)), dma((ZN,)),
        ],
        compiler_params=pltpu.CompilerParams(
            collective_id=cid, has_side_effects=True, vmem_limit_bytes=67043328
        ),
        name="scatter_all",
    )(grads.reshape((ZN, 2, 2, tiles) + box), note)


def layout():
    return [
        ("cls", 1, (D,)),
        ("mask_tok", 1, (D,)),
        ("b_pe", 1, (D,)),
        ("ln1_g", 1, (D,)),
        ("ln1_b", 1, (D,)),
        ("b_out", 1, (D,)),
        ("ln2_g", 1, (D,)),
        ("ln2_b", 1, (D,)),
        ("b_two", 1, (D,)),
        ("lnf_g", 1, (D,)),
        ("lnf_b", 1, (D,)),
        ("b_head", 1, (D,)),
        ("b_one", FF // D, (FF,)),
        ("w_pe", PP, (PP, D)),
        ("w_qkv", 3 * D, (D, 3 * D)),
        ("w_out", D, (D, D)),
        ("w_one", FF, (D, FF)),
        ("w_two", FF, (FF, D)),
        ("w_head", D, (D, D)),
    ]


def unpack(flat):
    tables = {}
    offset = 0
    for entry_name, entry_rows, entry_shape in layout():
        tables[entry_name] = flat[offset : offset + entry_rows].reshape(entry_shape)
        offset = offset + entry_rows
    return tables


def pack_flat(tables, total_rows):
    pieces = [tables[entry_name].reshape(-1, D) for entry_name, entry_rows, entry_shape in layout()]
    stacked = jnp.concatenate(pieces, 0)
    return jnp.concatenate(
        [stacked, jnp.zeros((total_rows - stacked.shape[0], D), stacked.dtype)], 0
    )


def reorder(stored, order):
    return stored.reshape(order.shape[0], -1, D)[order].reshape(-1, D)


def slot_info(split_rows, seq_side):
    column = jnp.arange(SL)[None, :]
    split_col = split_rows[:, None]
    first_side = seq_side == 0
    first_slot = jnp.where(first_side, 1, 0)
    filled = jnp.where(first_side, split_col * GRID, (GRID - split_col) * GRID)
    offset = jnp.where(first_side, -1, split_col * GRID)
    is_patch = (column >= first_slot) & (column < first_slot + filled)
    is_cls = first_side & (column == 0) & (split_col >= 0)
    grid_cell = jnp.clip(column + offset, 0, GRID * GRID - 1)
    return (is_patch, is_cls, grid_cell)


def sincos(grid_cell):
    quarter = D // 4
    frequency = 1.0 / 10000.0 ** (jnp.arange(quarter).astype(jnp.float32) / quarter)
    rows_at = (grid_cell // GRID).astype(jnp.float32)[..., None] * frequency
    cols_at = (grid_cell % GRID).astype(jnp.float32)[..., None] * frequency
    return jnp.concatenate(
        [jnp.sin(rows_at), jnp.cos(rows_at), jnp.sin(cols_at), jnp.cos(cols_at)], -1
    )


def layer_norm(values):
    center = jnp.mean(values, -1, keepdims=True)
    centred = values - center
    return centred * lax.rsqrt(jnp.mean(centred * centred, -1, keepdims=True) + NORM_EPS)


def matmul_f32(left_mat, right_mat):
    return jnp.dot(left_mat, right_mat, preferred_element_type=jnp.float32)


def weight_grad(left_mat, right_mat):
    return lax.dot_general(
        left_mat, right_mat, (((0,), (0,)), ((), ())), preferred_element_type=jnp.float32
    )


def back_dot(left_mat, right_mat):
    return lax.dot_general(
        left_mat, right_mat, (((1,), (1,)), ((), ())), preferred_element_type=jnp.float32
    )


def vector(params, entry_name):
    return params[entry_name].astype(jnp.float32)


def column_sums(values):
    return jnp.sum(values.astype(jnp.float32), 0)


def norm_fwd(values, gain_vec, bias_vec):
    center = jnp.mean(values, -1, keepdims=True)
    centred = values - center
    inverse = lax.rsqrt(jnp.mean(centred * centred, -1, keepdims=True) + NORM_EPS)
    normed = centred * inverse
    return (normed * gain_vec + bias_vec, normed, inverse)


def norm_back(grad_out, normed, inverse, gain_vec):
    scaled = grad_out * gain_vec
    grad_in = inverse * (
        scaled
        - jnp.mean(scaled, -1, keepdims=True)
        - normed * jnp.mean(scaled * normed, -1, keepdims=True)
    )
    return (grad_in, jnp.sum(grad_out * normed, 0), jnp.sum(grad_out, 0))


def place_tokens(params, embedded, is_patch, is_cls, hidden_mask, position):
    on_grid = embedded.reshape(is_patch.shape + (D,)) + position
    tokens = jnp.where(is_patch[..., None], on_grid, 0.0)
    tokens = jnp.where(hidden_mask[..., None], vector(params, "mask_tok") + position, tokens)
    tokens = jnp.where(is_cls[..., None], vector(params, "cls"), tokens)
    return tokens.reshape(-1, D)


def project(params, tokens, length):
    normed_in, normed, inverse = norm_fwd(tokens, vector(params, "ln1_g"), vector(params, "ln1_b"))
    normed_in = normed_in.astype(jnp.bfloat16)
    packed = (
        matmul_f32(normed_in, params["w_qkv"])
        .astype(jnp.bfloat16)
        .reshape(-1, length, 3, HEADS, HD)
    )
    return (normed_in, normed, inverse, packed[:, :, 0], packed[:, :, 1], packed[:, :, 2])


def scores_of(queries, keys_block, key_live):
    raw_scores = jnp.einsum(
        "bqhd,bkhd->bhqk", queries, keys_block, preferred_element_type=jnp.float32
    ) * HD ** (-0.5)
    return jnp.where(key_live[:, None, None, :], raw_scores, -1e30)


def attend(queries, blocks):
    scores = [scores_of(queries, block[0], block[2]) for block in blocks]
    highest = reduce_max([jnp.max(member, -1, keepdims=True) for member in scores])
    summed = sum([jnp.sum(jnp.exp(member - highest), -1, keepdims=True) for member in scores])
    logsum = highest + jnp.log(summed)
    mixed_out = sum(
        [
            jnp.einsum(
                "bhqk,bkhd->bqhd",
                jnp.exp(member - logsum).astype(jnp.bfloat16),
                block[1],
                preferred_element_type=jnp.float32,
            )
            for member, block in zip(scores, blocks)
        ]
    )
    return (mixed_out.astype(jnp.bfloat16).reshape(-1, D), logsum)


def reduce_max(members):
    highest = members[0]
    for member in members[1:]:
        highest = jnp.maximum(highest, member)
    return highest


def finish(params, tokens, queries, blocks):
    mixed_out, logsum = attend(queries, blocks)
    hidden = tokens + matmul_f32(mixed_out, params["w_out"]) + vector(params, "b_out")
    normed_two_in, normed_two, inverse_two = norm_fwd(
        hidden, vector(params, "ln2_g"), vector(params, "ln2_b")
    )
    normed_two_in = normed_two_in.astype(jnp.bfloat16)
    upward = matmul_f32(normed_two_in, params["w_one"]) + vector(params, "b_one")
    gelled = jax.nn.gelu(upward).astype(jnp.bfloat16)
    output = hidden + matmul_f32(gelled, params["w_two"]) + vector(params, "b_two")
    return (output, (mixed_out, logsum, normed_two, inverse_two, normed_two_in, upward, gelled))


def layer_back(params, grad_out, saved, far_blocks, key_live, gradients):
    (
        normed_in,
        normed,
        inverse,
        queries,
        keys_loc,
        values_loc,
        mixed_out,
        logsum,
        normed_two,
        inverse_two,
        normed_two_in,
        upward,
        gelled,
    ) = saved
    length = queries.shape[1]
    blocks = [(keys_loc, values_loc, key_live)] + far_blocks
    grad_branch = grad_out.astype(jnp.bfloat16)
    gradients["w_two"] = weight_grad(gelled, grad_branch)
    gradients["b_two"] = column_sums(grad_branch)
    unused, gelu_pull = jax.vjp(jax.nn.gelu, upward)
    grad_up = gelu_pull(back_dot(grad_branch, params["w_two"]))[0].astype(jnp.bfloat16)
    gradients["w_one"] = weight_grad(normed_two_in, grad_up)
    gradients["b_one"] = column_sums(grad_up)
    grad_two, gradients["ln2_g"], gradients["ln2_b"] = norm_back(
        back_dot(grad_up, params["w_one"]), normed_two, inverse_two, vector(params, "ln2_g")
    )
    grad_hidden = grad_out + grad_two
    grad_attn = grad_hidden.astype(jnp.bfloat16)
    gradients["w_out"] = weight_grad(mixed_out, grad_attn)
    gradients["b_out"] = column_sums(grad_attn)
    grad_mixed = (
        back_dot(grad_attn, params["w_out"]).astype(jnp.bfloat16).reshape(-1, length, HEADS, HD)
    )
    probs = [jnp.exp(scores_of(queries, block[0], block[2]) - logsum) for block in blocks]
    pushes = [
        jnp.einsum("bqhd,bkhd->bhqk", grad_mixed, block[1], preferred_element_type=jnp.float32)
        for block in blocks
    ]
    common = sum([jnp.sum(prob * push, -1, keepdims=True) for prob, push in zip(probs, pushes)])
    grad_scores = [
        (prob * (push - common)).astype(jnp.bfloat16) for prob, push in zip(probs, pushes)
    ]
    key_scale = HD ** (-0.5)
    grad_queries = (
        sum(
            [
                jnp.einsum("bhqk,bkhd->bqhd", member, block[0], preferred_element_type=jnp.float32)
                for member, block in zip(grad_scores, blocks)
            ]
        )
        * key_scale
    )
    key_grads = [
        jnp.einsum("bhqk,bqhd->bkhd", member, queries, preferred_element_type=jnp.float32)
        * key_scale
        for member in grad_scores
    ]
    value_grads = [
        jnp.einsum(
            "bhqk,bqhd->bkhd",
            prob.astype(jnp.bfloat16),
            grad_mixed,
            preferred_element_type=jnp.float32,
        )
        for prob in probs
    ]
    grad_keys, grad_values = (key_grads[0], value_grads[0])
    returned = from_partner(
        jnp.stack([key_grads[1], value_grads[1]]).astype(jnp.bfloat16), "seq", 0
    ).astype(jnp.float32)
    grad_keys = grad_keys + returned[0]
    grad_values = grad_values + returned[1]
    grad_packed = (
        jnp.stack([grad_queries, grad_keys, grad_values], 2).astype(jnp.bfloat16).reshape(-1, 3 * D)
    )
    gradients["w_qkv"] = weight_grad(normed_in, grad_packed)
    grad_first, gradients["ln1_g"], gradients["ln1_b"] = norm_back(
        back_dot(grad_packed, params["w_qkv"]), normed, inverse, vector(params, "ln1_g")
    )
    return grad_hidden + grad_first


def on_device(
    patches,
    block_masks,
    split_rows,
    span_order,
    weights,
    teacher,
    first_moment,
    second_moment,
    step_count,
):
    dp = lax.axis_size("dp")
    own_kernels = dp == 4 * ZN
    chip_count = jnp.sum((block_masks == 1).astype(jnp.float32))
    blocks_in = lambda rows: rows.reshape(-1, CR, D)
    if own_kernels:
        gathered, teacher_all, counts = gather_all(
            [
                blocks_in(weights.astype(jnp.bfloat16)),
                blocks_in(teacher),
                jnp.broadcast_to(chip_count, (4, 8, 128)),
            ],
            dp,
            1,
        )
        masked_count = jnp.sum(counts[:, 0, 0, 0])
        gathered, teacher_all = (gathered.reshape(-1, CR, D), teacher_all.reshape(-1, CR, D))
    else:
        gathered, teacher_all = (
            blocks_in(lax.all_gather(weights.astype(jnp.bfloat16), "dp", axis=0, tiled=True)),
            blocks_in(lax.all_gather(teacher, "dp", axis=0, tiled=True)),
        )
        masked_count = lax.psum(chip_count, "dp")
    inverse_order = jnp.argsort(span_order)
    params = unpack(gathered[inverse_order].reshape(-1, D))
    teacher_params = unpack(teacher_all[inverse_order].reshape(-1, D))
    seq_side = lax.axis_index("seq")
    is_patch, is_cls, grid_cell = slot_info(split_rows, seq_side)
    far_patch, far_cls, far_cell = slot_info(split_rows, 1 - seq_side)
    far_live = far_patch | far_cls
    length = SL
    images = patches.shape[0]
    hidden_mask = (jnp.take_along_axis(block_masks, grid_cell, 1) == 1) & is_patch
    key_live = is_patch | is_cls
    position = sincos(grid_cell)
    pixels = patches.reshape(-1, PP)
    embedded_teacher = matmul_f32(pixels, teacher_params["w_pe"]) + vector(teacher_params, "b_pe")
    embedded_student = matmul_f32(pixels, params["w_pe"]) + vector(params, "b_pe")
    tokens_teacher = place_tokens(
        teacher_params, embedded_teacher, is_patch, is_cls, jnp.zeros_like(hidden_mask), position
    )
    tokens_student = place_tokens(params, embedded_student, is_patch, is_cls, hidden_mask, position)
    teacher_proj = project(teacher_params, tokens_teacher, length)
    student_proj = project(params, tokens_student, length)
    arrived = from_partner(
        jnp.stack([teacher_proj[4], teacher_proj[5], student_proj[4], student_proj[5]]), "seq", 0
    )
    teacher_far = [(arrived[0], arrived[1], far_live)]
    student_far = [(arrived[2], arrived[3], far_live)]
    teacher_out, unused = finish(
        teacher_params,
        tokens_teacher,
        teacher_proj[3],
        [(teacher_proj[4], teacher_proj[5], key_live)] + teacher_far,
    )
    target = layer_norm(teacher_out)
    student_out, finish_saved = finish(
        params,
        tokens_student,
        student_proj[3],
        [(student_proj[4], student_proj[5], key_live)] + student_far,
    )
    final_in, final_normed, final_inverse = norm_fwd(
        student_out, vector(params, "lnf_g"), vector(params, "lnf_b")
    )
    final_in = final_in.astype(jnp.bfloat16)
    predicted = matmul_f32(final_in, params["w_head"]) + vector(params, "b_head")
    difference = predicted - target
    magnitude = jnp.abs(difference)
    elementwise = jnp.where(
        magnitude < BETA, 0.5 * difference * difference / BETA, magnitude - 0.5 * BETA
    )
    selected = hidden_mask.reshape(-1)[:, None]
    loss_scale = 1.0 / (math.sqrt(D) * masked_count)
    part_loss = jnp.sum(jnp.where(selected, elementwise, 0.0)) * loss_scale
    grad_pred = (
        jnp.where(selected, jnp.clip(difference / BETA, -1.0, 1.0), 0.0) * loss_scale
    ).astype(jnp.bfloat16)
    gradients = {}
    gradients["w_head"] = weight_grad(final_in, grad_pred)
    gradients["b_head"] = column_sums(grad_pred)
    grad_tokens, gradients["lnf_g"], gradients["lnf_b"] = norm_back(
        back_dot(grad_pred, params["w_head"]), final_normed, final_inverse, vector(params, "lnf_g")
    )
    saved = tuple(student_proj) + tuple(finish_saved)
    grad_tokens = layer_back(params, grad_tokens, saved, student_far, key_live, gradients)
    grad_slots = grad_tokens.reshape(images, length, D)
    visible = (is_patch & jnp.logical_not(hidden_mask))[..., None]
    grad_embed = jnp.where(visible, grad_slots, 0.0).astype(jnp.bfloat16).reshape(-1, D)
    gradients["w_pe"] = weight_grad(pixels, grad_embed)
    gradients["b_pe"] = column_sums(grad_embed)
    gradients["mask_tok"] = jnp.sum(jnp.where(hidden_mask[..., None], grad_slots, 0.0), (0, 1))
    gradients["cls"] = jnp.sum(jnp.where(is_cls[..., None], grad_slots, 0.0), (0, 1))
    stored_grad = reorder(pack_flat(gradients, span_order.shape[0] * CR), span_order)
    if own_kernels:
        owned_grad, totals = scatter_all(
            stored_grad.reshape(dp, -1, 8, D), jnp.broadcast_to(part_loss, (8, 128)), 2
        )
        owned_grad = owned_grad.reshape(-1, D)
        total_loss, squares = (totals[0, 0], totals[1, 0])
    else:
        owned_grad = lax.psum_scatter(stored_grad, "dp", scatter_dimension=0, tiled=True)
        owned_grad = lax.psum(owned_grad, "seq")
        total_loss = lax.psum(part_loss, ("dp", "seq"))
        squares = lax.psum(jnp.sum(owned_grad * owned_grad), "dp")
    grad_norm = jnp.sqrt(squares)
    clipped = owned_grad * (CLIP / jnp.maximum(grad_norm, CLIP))
    updated_first = BETA_ONE * first_moment + (1.0 - BETA_ONE) * clipped
    updated_second = BETA_TWO * second_moment + (1.0 - BETA_TWO) * clipped * clipped
    steps_done = step_count[0].astype(jnp.float32)
    adam_step = (
        updated_first
        / (1.0 - BETA_ONE**steps_done)
        / (jnp.sqrt(updated_second / (1.0 - BETA_TWO**steps_done)) + ADAM_EPS)
    )
    updated_weights = weights - LEARN * (adam_step + DECAY * weights)
    return (
        total_loss,
        grad_norm,
        updated_weights,
        updated_weights.astype(jnp.bfloat16),
        updated_first,
        updated_second,
    )


def solution(mesh):
    placed = (
        P("dp", "seq", None),
        P("dp", None),
        P("dp"),
        P(),
        P("dp", None),
        P("dp", None),
        P("dp", None),
        P("dp", None),
        P(),
    )
    return jax.shard_map(
        on_device,
        mesh=mesh,
        in_specs=placed,
        out_specs=(P(), P(), P("dp", None), P("dp", None), P("dp", None), P("dp", None)),
        check_vma=False,
    )
```

```python
import functools
import math

import jax
import jax.numpy as jnp
from jax import lax
from jax.experimental import pallas as pl
from jax.experimental.pallas import tpu as pltpu
from jax.sharding import PartitionSpec as P

D = 768
HEADS = 12
HD = 64
FF = 3072
PP = 768
GRID = 14
SL = 128
CR = 4


BETA = 2.0
CLIP = 0.01
LEARN = 0.03
DECAY = 0.05
BETA_ONE = 0.9
BETA_TWO = 0.999
ADAM_EPS = 1e-08
NORM_EPS = 1e-06


def from_partner(shard, axis, bit):
    return lax.ppermute(shard, axis, [(i, i ^ 1 << bit) for i in range(lax.axis_size(axis))])


MESH = pl.DeviceIdType.MESH
ZN = 4


def place():
    p = lax.axis_index("dp")
    return p, p // 4, (p // 2) % 2, p % 2, lax.axis_index("seq")


def to_chip(p, s):
    return (p, s)


def greet(p, z, s):
    barrier = pltpu.get_barrier_semaphore()

    def hello(dev):
        pl.semaphore_signal(barrier, inc=1, device_id=dev, device_id_type=MESH)

    hello((p, 1 - s))
    hello((p ^ 1, s))
    hello((p ^ 2, s))

    @pl.when(z > 0)
    def _():
        hello((p - 4, s))

    @pl.when(z < ZN - 1)
    def _():
        hello((p + 4, s))

    ends = jnp.where(z == 0, 1, 0) + jnp.where(z == ZN - 1, 1, 0)
    pl.semaphore_wait(barrier, 5 - ends)


def gather_kernel(nq, nk, *refs):
    src = refs[:nq]
    out = refs[nq : 2 * nq]
    send_sem, recv_sem, psend_sem, precv_sem, own_sem = refs[2 * nq :]
    p, z, y, x, s = place()

    def span(q, k, side):
        half = src[q].shape[0] // 2
        low, high = half * k // nk, half * (k + 1) // nk
        return pl.ds(side * half + low, high - low)

    def rows(q, k):
        return span(q, k, s)

    def far_rows(q, k):
        return span(q, k, 1 - s)

    def dest(way):
        if way == "u":
            return p + 4
        if way == "d":
            return p - 4
        return p ^ 1 if way == "x" else p ^ 2

    LANE = {"u": 0, "d": 1, "x": 2, "y": 3}

    def copy(q, k, origin, way, own):
        block = src[q].at[rows(q, k)] if own else out[q].at[origin, rows(q, k)]
        return pltpu.make_async_remote_copy(
            src_ref=block,
            dst_ref=out[q].at[origin, rows(q, k)],
            send_sem=send_sem.at[LANE[way], q, k, origin],
            recv_sem=recv_sem.at[q, k, origin],
            device_id=(dest(way), s),
            device_id_type=MESH,
        )

    def arrive(q, k, origin):
        pltpu.make_async_remote_copy(
            src_ref=out[q].at[origin, rows(q, k)],
            dst_ref=out[q].at[origin, rows(q, k)],
            send_sem=send_sem.at[0, q, k, origin],
            recv_sem=recv_sem.at[q, k, origin],
            device_id=(p, s),
            device_id_type=MESH,
        ).wait_recv()

    def hand(q, k, origin):
        return pltpu.make_async_remote_copy(
            src_ref=out[q].at[origin, rows(q, k)],
            dst_ref=out[q].at[origin, rows(q, k)],
            send_sem=psend_sem.at[q, k, origin],
            recv_sem=precv_sem.at[q, k, origin],
            device_id=(p, 1 - s),
            device_id_type=MESH,
        )

    greet(p, z, s)
    pieces = [(q, k) for q in range(nq) for k in range(nk)]
    first = lambda k: "x" if k % 2 == 0 else "y"
    second = lambda k: "y" if k % 2 == 0 else "x"
    log = []

    def go(cond, fn):
        if cond is None:
            fn()
        else:
            pl.when(cond)(fn)

    def start(cond, c):
        go(cond, c.start)
        log.append((cond, c.wait_send))

    def both(a, b):
        return b if a is None else a & b

    for q, k in pieces:
        start(z < ZN - 1, copy(q, k, p, "u", True))
        start(z > 0, copy(q, k, p, "d", True))
        start(None, copy(q, k, p, first(k), True))
        start(None, copy(q, k, p, second(k), True))
    owned = [pltpu.make_async_copy(src[q], out[q].at[p], own_sem.at[q]) for q in range(nq)]
    for c in owned:
        c.start()

    offsets = [0]
    for d in range(1, ZN):
        offsets += [-d, d]
    for q in range(nq):
        for d in offsets:
            ok = None if d == 0 else ((z + d >= 0) & (z + d < ZN))
            o = p + 4 * d
            for k in range(nk):
                if d != 0:
                    def relay(k=k, o=o, d=d):
                        arrive(q, k, o)

                    go(ok, relay)
                    if d < 0:
                        start(both(ok, z < ZN - 1), copy(q, k, o, "u", False))
                    else:
                        start(both(ok, z > 0), copy(q, k, o, "d", False))
                    start(ok, copy(q, k, o, first(k), False))
                    start(ok, copy(q, k, o, second(k), False))
                    start(ok, hand(q, k, o))
            for k in range(nk):
                o1 = (p ^ (1 if first(k) == "x" else 2)) + 4 * d
                go(ok, lambda: arrive(q, k, o1))
                start(ok, copy(q, k, o1, second(k), False))
                start(ok, hand(q, k, o1))
            for k in range(nk):
                o2 = (p ^ (2 if first(k) == "x" else 1)) + 4 * d
                go(ok, lambda: arrive(q, k, o2))
                start(ok, hand(q, k, o2))
            for k in range(nk):
                o3 = (p ^ 3) + 4 * d
                go(ok, lambda: arrive(q, k, o3))
                start(ok, hand(q, k, o3))
    for c in owned:
        c.wait()
    for cond, w in log:
        go(cond, w)
    for q in range(nq):
        for k in range(nk):
            for flip in range(4):
                for d in offsets:
                    if d == 0 and flip == 0:
                        continue
                    ok = None if d == 0 else ((z + d >= 0) & (z + d < ZN))
                    o = (p ^ flip) + 4 * d

                    def take(q=q, k=k, o=o):
                        pltpu.make_async_remote_copy(
                            src_ref=out[q].at[o, far_rows(q, k)],
                            dst_ref=out[q].at[o, far_rows(q, k)],
                            send_sem=psend_sem.at[q, k, o],
                            recv_sem=precv_sem.at[q, k, o],
                            device_id=(p, 1 - s),
                            device_id_type=MESH,
                        ).wait_recv()

                    go(ok, take)


def gather_all(shards, dp, cid, nk=2):
    nq = len(shards)
    shapes = [jax.ShapeDtypeStruct((dp,) + shard.shape, shard.dtype) for shard in shards]
    return pl.pallas_call(
        functools.partial(gather_kernel, nq, nk),
        out_shape=shapes,
        in_specs=[pl.BlockSpec(memory_space=pltpu.VMEM)] * nq,
        out_specs=[pl.BlockSpec(memory_space=pl.ANY)] * nq,
        scratch_shapes=[
            pltpu.SemaphoreType.DMA((4, nq, nk, dp)),
            pltpu.SemaphoreType.DMA((nq, nk, dp)),
            pltpu.SemaphoreType.DMA((nq, nk, dp)),
            pltpu.SemaphoreType.DMA((nq, nk, dp)),
            pltpu.SemaphoreType.DMA((nq,)),
        ],
        compiler_params=pltpu.CompilerParams(
            collective_id=cid, has_side_effects=True, vmem_limit_bytes=60 * 2**20
        ),
        name="gather_all",
    )(*shards)


def scatter_kernel(cuts, g_ref, note_ref, out_ref, tot_ref, acc, pr, r1, r2, ru, rd,
                   sbuf, rbuf, zbuf, loc_sem, pair_s, pair_r, d1_s, d1_r, d2_s, d2_r,
                   up_s, up_r, dn_s, dn_r, fin_s, fin_r, sc_s, sc_r, zu_s, zu_r, zd_s, zd_r):
    p, z, y, x, s = place()
    H = cuts[-1]
    over = 2 * H - out_ref.shape[0]
    base = s * (H - over)
    far = (1 - s) * (H - over)
    nk = len(cuts) - 1

    def rows(k, first=0):
        return pl.ds(first + cuts[k], cuts[k + 1] - cuts[k])

    def remote(src, dst, a, b, dev):
        return pltpu.make_async_remote_copy(src_ref=src, dst_ref=dst, send_sem=a, recv_sem=b,
                                            device_id=dev, device_id_type=MESH)

    def load(k):
        return pltpu.make_async_copy(g_ref.at[:, :, :, rows(k, base)],
                                     acc.at[:, :, :, rows(k)], loc_sem.at[k])

    def pair(k):
        return remote(g_ref.at[:, :, :, rows(k, far)], pr.at[:, :, :, rows(k)],
                      pair_s.at[k], pair_r.at[k], (p, 1 - s))

    def one(k):
        if k % 2 == 0:
            src, dst, dev = acc.at[:, :, 1 - x, rows(k)], r1.at[:, :, rows(k)], (p ^ 1, s)
        else:
            src, dst, dev = acc.at[:, 1 - y, :, rows(k)], r1.at[:, :, rows(k)], (p ^ 2, s)
        return remote(src, dst, d1_s.at[k], d1_r.at[k], dev)

    def two(k):
        if k % 2 == 0:
            src, dev = acc.at[:, 1 - y, x, rows(k)], (p ^ 2, s)
        else:
            src, dev = acc.at[:, y, 1 - x, rows(k)], (p ^ 1, s)
        return remote(src, r2.at[:, rows(k)], d2_s.at[k], d2_r.at[k], dev)

    def up(k, t):
        return remote(acc.at[t, y, x, rows(k)], ru.at[t, rows(k)], up_s.at[k, t], up_r.at[k, t],
                      (p + 4, s))

    def down(k, t):
        return remote(acc.at[t, y, x, rows(k)], rd.at[t, rows(k)], dn_s.at[k, t], dn_r.at[k, t],
                      (p - 4, s))

    def add_up(k, t):
        acc[t, y, x, rows(k)] += ru[t, rows(k)]

    def add_down(k, t):
        acc[t, y, x, rows(k)] += rd[t, rows(k)]

    greet(p, z, s)
    for k in range(nk):
        pair(k).start()
        load(k).start()

    def stage_pair(k):
        load(k).wait()
        pair(k).wait_recv()

        def body(i, c):
            a, b, d = i // 4, (i // 2) % 2, i % 2
            acc[a, b, d, rows(k)] += pr[a, b, d, rows(k)]
            return c

        lax.fori_loop(0, 16, body, 0)
        one(k).start()

    def stage_one(k):
        one(k).wait_recv()

        def body(i, c):
            a, b = i // 2, i % 2
            if k % 2 == 0:
                acc[a, b, x, rows(k)] += r1[a, b, rows(k)]
            else:
                acc[a, y, b, rows(k)] += r1[a, b, rows(k)]
            return c

        lax.fori_loop(0, 8, body, 0)
        two(k).start()

    def stage_two(k):
        two(k).wait_recv()

        def body(a, c):
            acc[a, y, x, rows(k)] += r2[a, rows(k)]
            return c

        lax.fori_loop(0, 4, body, 0)

        @pl.when(z == 0)
        def _():
            for t in range(ZN - 1, 0, -1):
                up(k, t).start()

        @pl.when(z == ZN - 1)
        def _():
            for t in range(ZN - 1):
                down(k, t).start()

    def stage_z(k, i):
        t = ZN - 1 - i

        @pl.when((z > 0) & (z < t))
        def _():
            up(k, t).wait_recv()
            add_up(k, t)
            up(k, t).start()

        @pl.when((z < ZN - 1) & (z > i))
        def _():
            down(k, i).wait_recv()
            add_down(k, i)
            down(k, i).start()

    def stage_last(k):
        @pl.when(z > 0)
        def _():
            up(k, z).wait_recv()
            add_up(k, z)

        @pl.when(z < ZN - 1)
        def _():
            down(k, z).wait_recv()
            add_down(k, z)

    stages = [stage_pair, stage_one, stage_two] + [
        functools.partial(lambda i, k: stage_z(k, i), i) for i in range(ZN - 1)
    ] + [stage_last]
    for t in range(nk + len(stages) - 1):
        for j in range(len(stages)):
            if 0 <= t - j < nk:
                stages[j](t - j)

    low = lambda: remote(acc.at[z, y, x, pl.ds(0, H)], out_ref.at[pl.ds(0, H)],
                         fin_s, fin_r, (p, 1 - s))
    high = lambda: remote(acc.at[z, y, x, pl.ds(over, H - over)],
                          out_ref.at[pl.ds(H, H - over)], fin_s, fin_r, (p, 1 - s))

    @pl.when(s == 0)
    def _():
        low().start()
        out_ref[pl.ds(0, H)] = acc[z, y, x, pl.ds(0, H)]

    @pl.when(s == 1)
    def _():
        high().start()
        out_ref[pl.ds(H, H - over)] = acc[z, y, x, pl.ds(over, H - over)]

    mine = acc[z, y, x, pl.ds(over, H - over)]
    sq = jnp.sum(mine * mine)
    for i in range(over):
        head = acc[z, y, x, i]
        sq = sq + jnp.where(s == 0, jnp.sum(head * head), 0.0)
    row = lax.broadcasted_iota(jnp.int32, (8, 128), 0)
    cur = jnp.where(row == 1, sq, note_ref[...])
    for j, dev in enumerate([(p, 1 - s), (p ^ 1, s), (p ^ 2, s)]):
        sbuf[j] = cur
        c = remote(sbuf.at[j], rbuf.at[j], sc_s.at[j], sc_r.at[j], dev)
        c.start()
        c.wait()
        cur = cur + rbuf[j]
    zbuf[z] = cur

    def zup(o):
        return remote(zbuf.at[o], zbuf.at[o], zu_s.at[o], zu_r.at[o], (p + 4, s))

    def zdn(o):
        return remote(zbuf.at[o], zbuf.at[o], zd_s.at[o], zd_r.at[o], (p - 4, s))

    @pl.when(z < ZN - 1)
    def _():
        zup(z).start()

    @pl.when(z > 0)
    def _():
        zdn(z).start()

    for d in range(1, ZN):
        @pl.when(z - d >= 0)
        def _():
            zup(z - d).wait_recv()

        @pl.when((z - d >= 0) & (z < ZN - 1))
        def _():
            zup(z - d).start()

        @pl.when(z + d < ZN)
        def _():
            zdn(z + d).wait_recv()

        @pl.when((z + d < ZN) & (z > 0))
        def _():
            zdn(z + d).start()

    total = zbuf[0]
    for i in range(1, ZN):
        total = total + zbuf[i]
    tot_ref[...] = total

    @pl.when(s == 0)
    def _():
        low().wait_send()
        high().wait_recv()

    @pl.when(s == 1)
    def _():
        high().wait_send()
        low().wait_recv()

    for k in range(nk):
        pair(k).wait_send()
        one(k).wait_send()
        two(k).wait_send()
        for t in range(ZN):
            @pl.when(z < t)
            def _():
                up(k, t).wait_send()

            @pl.when(z > t)
            def _():
                down(k, t).wait_send()
    for o in range(ZN):
        @pl.when((o <= z) & (z < ZN - 1))
        def _():
            zup(o).wait_send()

        @pl.when((o >= z) & (z > 0))
        def _():
            zdn(o).wait_send()


def scatter_all(grads, note, cid, nk=6):
    dp, tiles = grads.shape[0], grads.shape[1]
    H = (tiles + 1) // 2
    cuts = [H * i // nk for i in range(nk + 1)]
    dma = pltpu.SemaphoreType.DMA
    box = (8, D)
    return pl.pallas_call(
        functools.partial(scatter_kernel, cuts),
        out_shape=[
            jax.ShapeDtypeStruct((tiles,) + box, jnp.float32),
            jax.ShapeDtypeStruct((8, 128), jnp.float32),
        ],
        in_specs=[pl.BlockSpec(memory_space=pl.ANY), pl.BlockSpec(memory_space=pltpu.VMEM)],
        out_specs=[pl.BlockSpec(memory_space=pltpu.VMEM)] * 2,
        scratch_shapes=[
            pltpu.VMEM((ZN, 2, 2, H) + box, jnp.float32),
            pltpu.VMEM((ZN, 2, 2, H) + box, jnp.float32),
            pltpu.VMEM((ZN, 2, H) + box, jnp.float32),
            pltpu.VMEM((ZN, H) + box, jnp.float32),
            pltpu.VMEM((ZN, H) + box, jnp.float32),
            pltpu.VMEM((ZN, H) + box, jnp.float32),
            pltpu.VMEM((3, 8, 128), jnp.float32),
            pltpu.VMEM((3, 8, 128), jnp.float32),
            pltpu.VMEM((ZN, 8, 128), jnp.float32),
            dma((nk,)), dma((nk,)), dma((nk,)), dma((nk,)), dma((nk,)), dma((nk,)), dma((nk,)),
            dma((nk, ZN)), dma((nk, ZN)), dma((nk, ZN)), dma((nk, ZN)),
            dma, dma, dma((3,)), dma((3,)), dma((ZN,)), dma((ZN,)), dma((ZN,)), dma((ZN,)),
        ],
        compiler_params=pltpu.CompilerParams(
            collective_id=cid, has_side_effects=True, vmem_limit_bytes=67043328
        ),
        name="scatter_all",
    )(grads.reshape((ZN, 2, 2, tiles) + box), note)


VECTORS = [
    "cls",
    "mask_tok",
    "b_pe",
    "ln1_g",
    "ln1_b",
    "b_out",
    "ln2_g",
    "ln2_b",
    "b_two",
    "lnf_g",
    "lnf_b",
    "b_head",
]
NARROW = [("small", 16, 1), ("w_pe", 768, 1), ("w_qkv", 2304, 3), ("w_out", 768, 1),
          ("w_one", 3072, 4), ("w_two", 3072, 1), ("w_head", 768, 1)]
LHS_T = (((0,), (0,)), ((), ()))


def sort_kernel(inv_ref, g_ref, small, pe, qkv, out, one, two, head, rows, wide):
    start = 0
    for (name, count, ways), dst in zip(NARROW, (small, pe, qkv, out, one, two, head)):
        to = dst if ways == 1 else rows

        def group(i, c, start=start, to=to):
            for q in range(4):
                to[i, 4 * q : 4 * q + 4, :] = g_ref[inv_ref[start // 4 + 4 * i + q]]
            return c

        lax.fori_loop(0, count // 16, group, 0)
        if ways > 1:
            def widen(i, c):
                r = pl.multiple_of(i * 64, 64)
                full = rows[pl.ds(i * 4, 4)].reshape(64, D).astype(jnp.float32)
                for n in range(D // 128):
                    wide[n, pl.ds(r, 64), :] = full[:, 128 * n : 128 * n + 128]
                return c

            lax.fori_loop(0, count // 64, widen, 0)
            high = count // ways
            for w in range(ways):
                for r in range(0, high, 128):
                    for n in range(D // 128):
                        piece = wide[n, pl.ds(r * ways + w, 128, stride=ways), :]
                        low = w * D + 128 * n
                        dst[pl.ds(r, 128), low : low + 128] = piece.astype(jnp.bfloat16)
        start += count


def sorted_weights(gathered, inverse):
    bf = jnp.bfloat16
    shapes = [(1, 16, D), (48, 16, D), (D, 3 * D), (48, 16, D), (D, FF), (192, 16, D), (48, 16, D)]
    outs = pl.pallas_call(
        sort_kernel,
        out_shape=[jax.ShapeDtypeStruct(s, bf) for s in shapes],
        in_specs=[pl.BlockSpec(memory_space=pltpu.SMEM), pl.BlockSpec(memory_space=pltpu.VMEM)],
        out_specs=[pl.BlockSpec(memory_space=pltpu.VMEM)] * 7,
        scratch_shapes=[pltpu.VMEM((192, 16, D), bf), pltpu.VMEM((D // 128, 3072, 128), jnp.float32)],
        compiler_params=pltpu.CompilerParams(vmem_limit_bytes=67043328),
        name="sort_weights",
    )(inverse, gathered)
    small = outs[0].reshape(16, D)
    tables = {name: small[i] for i, name in enumerate(VECTORS)}
    tables["b_one"] = small[12:].reshape(FF)
    tables["w_pe"] = outs[1].reshape(D, D)
    tables["w_qkv"] = outs[2]
    tables["w_out"] = outs[3].reshape(D, D)
    tables["w_one"] = outs[4]
    tables["w_two"] = outs[5].reshape(FF, D)
    tables["w_head"] = outs[6].reshape(D, D)
    return tables


def grad_kernel(order_ref, small, px, ge, a, gq, o, gr, a2, gu, gel, gz, fin, gp, out_ref,
                flat, buf, sem):
    total = flat.shape[1]
    cols = [(n, slice(128 * n, 128 * n + 128)) for n in range(D // 128)]
    for n, col in cols:
        flat[n, pl.ds(0, 16), :] = small[:, col]
    start = 16
    for lhs, rhs, ways in ((px, ge, 1), (a, gq, 3), (o, gr, 1), (a2, gu, 4), (gel, gz, 1), (fin, gp, 1)):
        depth = lhs.shape[1]

        def tile(i, c, lhs=lhs, rhs=rhs, ways=ways, start=start):
            left = lhs[:, pl.ds(pl.multiple_of(i * 256, 256), 256)]
            for w in range(ways):
                part = lax.dot_general(left, rhs[:, w * D : (w + 1) * D], LHS_T,
                                       preferred_element_type=jnp.float32)
                for n, col in cols:
                    if ways == 1:
                        flat[n, pl.ds(pl.multiple_of(start + i * 256, 8), 256), :] = part[:, col]
                    else:
                        first = start + i * 256 * ways + w
                        flat[n, pl.ds(first, 256, stride=ways), :] = part[:, col]
            return c

        lax.fori_loop(0, depth // 256, tile, 0)
        start += depth * ways
    for n, col in cols:
        flat[n, pl.ds(start, total - start), :] = jnp.zeros((total - start, 128), jnp.float32)
    owners, tiles = out_ref.shape[0], out_ref.shape[1]

    def put(n, slot):
        return pltpu.make_async_copy(buf.at[slot], out_ref.at[n], sem.at[slot])

    def owner(n, c):
        slot = n % 2

        @pl.when(n >= 2)
        def _():
            put(n - 2, slot).wait()

        def pair(t, c):
            for h in range(2):
                j = order_ref[(n * tiles + t) * 2 + h]
                for m, col in cols:
                    buf[slot, t, 4 * h : 4 * h + 4, col] = flat[m, pl.ds(4 * j, 4), :]
            return c

        lax.fori_loop(0, tiles, pair, 0)
        put(n, slot).start()
        return c

    lax.fori_loop(0, owners, owner, 0)
    put(owners - 2, (owners - 2) % 2).wait()
    put(owners - 1, (owners - 1) % 2).wait()


def packed_grads(order, small, pairs, dp):
    blocks = order.shape[0]
    tiles = blocks * CR // 8 // dp
    ops = [m for pair in pairs for m in pair]
    return pl.pallas_call(
        grad_kernel,
        out_shape=jax.ShapeDtypeStruct((dp, tiles, 8, D), jnp.float32),
        in_specs=[pl.BlockSpec(memory_space=pltpu.SMEM)]
        + [pl.BlockSpec(memory_space=pltpu.VMEM)] * (1 + len(ops)),
        out_specs=pl.BlockSpec(memory_space=pl.ANY),
        scratch_shapes=[
            pltpu.VMEM((D // 128, blocks * CR, 128), jnp.float32),
            pltpu.VMEM((2, tiles, 8, D), jnp.float32),
            pltpu.SemaphoreType.DMA((2,)),
        ],
        compiler_params=pltpu.CompilerParams(vmem_limit_bytes=67043328),
        name="pack_grads",
    )(order, small, *ops)


def slot_info(split_rows, seq_side):
    column = jnp.arange(SL)[None, :]
    split_col = split_rows[:, None]
    first_side = seq_side == 0
    first_slot = jnp.where(first_side, 1, 0)
    filled = jnp.where(first_side, split_col * GRID, (GRID - split_col) * GRID)
    offset = jnp.where(first_side, -1, split_col * GRID)
    is_patch = (column >= first_slot) & (column < first_slot + filled)
    is_cls = first_side & (column == 0) & (split_col >= 0)
    grid_cell = jnp.clip(column + offset, 0, GRID * GRID - 1)
    return (is_patch, is_cls, grid_cell)


def sincos(grid_cell):
    quarter = D // 4
    frequency = 1.0 / 10000.0 ** (jnp.arange(quarter).astype(jnp.float32) / quarter)
    rows_at = (grid_cell // GRID).astype(jnp.float32)[..., None] * frequency
    cols_at = (grid_cell % GRID).astype(jnp.float32)[..., None] * frequency
    return jnp.concatenate(
        [jnp.sin(rows_at), jnp.cos(rows_at), jnp.sin(cols_at), jnp.cos(cols_at)], -1
    )


def layer_norm(values):
    center = jnp.mean(values, -1, keepdims=True)
    centred = values - center
    return centred * lax.rsqrt(jnp.mean(centred * centred, -1, keepdims=True) + NORM_EPS)


def matmul_f32(left_mat, right_mat):
    return jnp.dot(left_mat, right_mat, preferred_element_type=jnp.float32)


def back_dot(left_mat, right_mat):
    return lax.dot_general(
        left_mat, right_mat, (((1,), (1,)), ((), ())), preferred_element_type=jnp.float32
    )


def vector(params, entry_name):
    return params[entry_name].astype(jnp.float32)


def column_sums(values):
    return jnp.sum(values.astype(jnp.float32), 0)


def norm_fwd(values, gain_vec, bias_vec):
    center = jnp.mean(values, -1, keepdims=True)
    centred = values - center
    inverse = lax.rsqrt(jnp.mean(centred * centred, -1, keepdims=True) + NORM_EPS)
    normed = centred * inverse
    return (normed * gain_vec + bias_vec, normed, inverse)


def norm_back(grad_out, normed, inverse, gain_vec):
    scaled = grad_out * gain_vec
    grad_in = inverse * (
        scaled
        - jnp.mean(scaled, -1, keepdims=True)
        - normed * jnp.mean(scaled * normed, -1, keepdims=True)
    )
    return (grad_in, jnp.sum(grad_out * normed, 0), jnp.sum(grad_out, 0))


def place_tokens(params, embedded, is_patch, is_cls, hidden_mask, position):
    on_grid = embedded.reshape(is_patch.shape + (D,)) + position
    tokens = jnp.where(is_patch[..., None], on_grid, 0.0)
    tokens = jnp.where(hidden_mask[..., None], vector(params, "mask_tok") + position, tokens)
    tokens = jnp.where(is_cls[..., None], vector(params, "cls"), tokens)
    return tokens.reshape(-1, D)


def project(params, tokens, length):
    normed_in, normed, inverse = norm_fwd(tokens, vector(params, "ln1_g"), vector(params, "ln1_b"))
    normed_in = normed_in.astype(jnp.bfloat16)
    packed = (
        matmul_f32(normed_in, params["w_qkv"])
        .astype(jnp.bfloat16)
        .reshape(-1, length, 3, HEADS, HD)
    )
    return (normed_in, normed, inverse, packed[:, :, 0], packed[:, :, 1], packed[:, :, 2])


def scores_of(queries, keys_block, key_live):
    raw_scores = jnp.einsum(
        "bqhd,bkhd->bhqk", queries, keys_block, preferred_element_type=jnp.float32
    ) * HD ** (-0.5)
    return jnp.where(key_live[:, None, None, :], raw_scores, -1e30)


def attend(queries, blocks):
    scores = [scores_of(queries, block[0], block[2]) for block in blocks]
    highest = reduce_max([jnp.max(member, -1, keepdims=True) for member in scores])
    summed = sum([jnp.sum(jnp.exp(member - highest), -1, keepdims=True) for member in scores])
    logsum = highest + jnp.log(summed)
    mixed_out = sum(
        [
            jnp.einsum(
                "bhqk,bkhd->bqhd",
                jnp.exp(member - logsum).astype(jnp.bfloat16),
                block[1],
                preferred_element_type=jnp.float32,
            )
            for member, block in zip(scores, blocks)
        ]
    )
    return (mixed_out.astype(jnp.bfloat16).reshape(-1, D), logsum)


def reduce_max(members):
    highest = members[0]
    for member in members[1:]:
        highest = jnp.maximum(highest, member)
    return highest


def finish(params, tokens, queries, blocks):
    mixed_out, logsum = attend(queries, blocks)
    hidden = tokens + matmul_f32(mixed_out, params["w_out"]) + vector(params, "b_out")
    normed_two_in, normed_two, inverse_two = norm_fwd(
        hidden, vector(params, "ln2_g"), vector(params, "ln2_b")
    )
    normed_two_in = normed_two_in.astype(jnp.bfloat16)
    upward = matmul_f32(normed_two_in, params["w_one"]) + vector(params, "b_one")
    gelled = jax.nn.gelu(upward).astype(jnp.bfloat16)
    output = hidden + matmul_f32(gelled, params["w_two"]) + vector(params, "b_two")
    return (output, (mixed_out, logsum, normed_two, inverse_two, normed_two_in, upward, gelled))


def layer_back(params, grad_out, saved, far_blocks, key_live, gradients):
    (
        normed_in,
        normed,
        inverse,
        queries,
        keys_loc,
        values_loc,
        mixed_out,
        logsum,
        normed_two,
        inverse_two,
        normed_two_in,
        upward,
        gelled,
    ) = saved
    length = queries.shape[1]
    blocks = [(keys_loc, values_loc, key_live)] + far_blocks
    grad_branch = grad_out.astype(jnp.bfloat16)
    gradients["w_two"] = (gelled, grad_branch)
    gradients["b_two"] = column_sums(grad_branch)
    unused, gelu_pull = jax.vjp(jax.nn.gelu, upward)
    grad_up = gelu_pull(back_dot(grad_branch, params["w_two"]))[0].astype(jnp.bfloat16)
    gradients["w_one"] = (normed_two_in, grad_up)
    gradients["b_one"] = column_sums(grad_up)
    grad_two, gradients["ln2_g"], gradients["ln2_b"] = norm_back(
        back_dot(grad_up, params["w_one"]), normed_two, inverse_two, vector(params, "ln2_g")
    )
    grad_hidden = grad_out + grad_two
    grad_attn = grad_hidden.astype(jnp.bfloat16)
    gradients["w_out"] = (mixed_out, grad_attn)
    gradients["b_out"] = column_sums(grad_attn)
    grad_mixed = (
        back_dot(grad_attn, params["w_out"]).astype(jnp.bfloat16).reshape(-1, length, HEADS, HD)
    )
    probs = [jnp.exp(scores_of(queries, block[0], block[2]) - logsum) for block in blocks]
    pushes = [
        jnp.einsum("bqhd,bkhd->bhqk", grad_mixed, block[1], preferred_element_type=jnp.float32)
        for block in blocks
    ]
    common = sum([jnp.sum(prob * push, -1, keepdims=True) for prob, push in zip(probs, pushes)])
    grad_scores = [
        (prob * (push - common)).astype(jnp.bfloat16) for prob, push in zip(probs, pushes)
    ]
    key_scale = HD ** (-0.5)
    grad_queries = (
        sum(
            [
                jnp.einsum("bhqk,bkhd->bqhd", member, block[0], preferred_element_type=jnp.float32)
                for member, block in zip(grad_scores, blocks)
            ]
        )
        * key_scale
    )
    key_grads = [
        jnp.einsum("bhqk,bqhd->bkhd", member, queries, preferred_element_type=jnp.float32)
        * key_scale
        for member in grad_scores
    ]
    value_grads = [
        jnp.einsum(
            "bhqk,bqhd->bkhd",
            prob.astype(jnp.bfloat16),
            grad_mixed,
            preferred_element_type=jnp.float32,
        )
        for prob in probs
    ]
    grad_keys, grad_values = (key_grads[0], value_grads[0])
    returned = from_partner(
        jnp.stack([key_grads[1], value_grads[1]]).astype(jnp.bfloat16), "seq", 0
    ).astype(jnp.float32)
    grad_keys = grad_keys + returned[0]
    grad_values = grad_values + returned[1]
    grad_packed = (
        jnp.stack([grad_queries, grad_keys, grad_values], 2).astype(jnp.bfloat16).reshape(-1, 3 * D)
    )
    gradients["w_qkv"] = (normed_in, grad_packed)
    grad_first, gradients["ln1_g"], gradients["ln1_b"] = norm_back(
        back_dot(grad_packed, params["w_qkv"]), normed, inverse, vector(params, "ln1_g")
    )
    return grad_hidden + grad_first


def on_device(
    patches,
    block_masks,
    split_rows,
    span_order,
    weights,
    teacher,
    first_moment,
    second_moment,
    step_count,
):
    dp = lax.axis_size("dp")
    own_kernels = dp == 4 * ZN
    chip_count = jnp.sum((block_masks == 1).astype(jnp.float32))
    blocks_in = lambda rows: rows.reshape(-1, CR, D)
    if own_kernels:
        gathered, teacher_all, counts = gather_all(
            [
                blocks_in(weights.astype(jnp.bfloat16)),
                blocks_in(teacher),
                jnp.broadcast_to(chip_count, (4, 8, 128)),
            ],
            dp,
            1,
        )
        masked_count = jnp.sum(counts[:, 0, 0, 0])
        gathered, teacher_all = (gathered.reshape(-1, CR, D), teacher_all.reshape(-1, CR, D))
    else:
        gathered, teacher_all = (
            blocks_in(lax.all_gather(weights.astype(jnp.bfloat16), "dp", axis=0, tiled=True)),
            blocks_in(lax.all_gather(teacher, "dp", axis=0, tiled=True)),
        )
        masked_count = lax.psum(chip_count, "dp")
    inverse_order = jnp.argsort(span_order)
    params = sorted_weights(gathered, inverse_order)
    teacher_params = sorted_weights(teacher_all, inverse_order)
    seq_side = lax.axis_index("seq")
    is_patch, is_cls, grid_cell = slot_info(split_rows, seq_side)
    far_patch, far_cls, far_cell = slot_info(split_rows, 1 - seq_side)
    far_live = far_patch | far_cls
    length = SL
    images = patches.shape[0]
    hidden_mask = (jnp.take_along_axis(block_masks, grid_cell, 1) == 1) & is_patch
    key_live = is_patch | is_cls
    position = sincos(grid_cell)
    pixels = patches.reshape(-1, PP)
    embedded_teacher = matmul_f32(pixels, teacher_params["w_pe"]) + vector(teacher_params, "b_pe")
    embedded_student = matmul_f32(pixels, params["w_pe"]) + vector(params, "b_pe")
    tokens_teacher = place_tokens(
        teacher_params, embedded_teacher, is_patch, is_cls, jnp.zeros_like(hidden_mask), position
    )
    tokens_student = place_tokens(params, embedded_student, is_patch, is_cls, hidden_mask, position)
    teacher_proj = project(teacher_params, tokens_teacher, length)
    student_proj = project(params, tokens_student, length)
    arrived = from_partner(
        jnp.stack([teacher_proj[4], teacher_proj[5], student_proj[4], student_proj[5]]), "seq", 0
    )
    teacher_far = [(arrived[0], arrived[1], far_live)]
    student_far = [(arrived[2], arrived[3], far_live)]
    teacher_out, unused = finish(
        teacher_params,
        tokens_teacher,
        teacher_proj[3],
        [(teacher_proj[4], teacher_proj[5], key_live)] + teacher_far,
    )
    target = layer_norm(teacher_out)
    student_out, finish_saved = finish(
        params,
        tokens_student,
        student_proj[3],
        [(student_proj[4], student_proj[5], key_live)] + student_far,
    )
    final_in, final_normed, final_inverse = norm_fwd(
        student_out, vector(params, "lnf_g"), vector(params, "lnf_b")
    )
    final_in = final_in.astype(jnp.bfloat16)
    predicted = matmul_f32(final_in, params["w_head"]) + vector(params, "b_head")
    difference = predicted - target
    magnitude = jnp.abs(difference)
    elementwise = jnp.where(
        magnitude < BETA, 0.5 * difference * difference / BETA, magnitude - 0.5 * BETA
    )
    selected = hidden_mask.reshape(-1)[:, None]
    loss_scale = 1.0 / (math.sqrt(D) * masked_count)
    part_loss = jnp.sum(jnp.where(selected, elementwise, 0.0)) * loss_scale
    grad_pred = (
        jnp.where(selected, jnp.clip(difference / BETA, -1.0, 1.0), 0.0) * loss_scale
    ).astype(jnp.bfloat16)
    gradients = {}
    gradients["w_head"] = (final_in, grad_pred)
    gradients["b_head"] = column_sums(grad_pred)
    grad_tokens, gradients["lnf_g"], gradients["lnf_b"] = norm_back(
        back_dot(grad_pred, params["w_head"]), final_normed, final_inverse, vector(params, "lnf_g")
    )
    saved = tuple(student_proj) + tuple(finish_saved)
    grad_tokens = layer_back(params, grad_tokens, saved, student_far, key_live, gradients)
    grad_slots = grad_tokens.reshape(images, length, D)
    visible = (is_patch & jnp.logical_not(hidden_mask))[..., None]
    grad_embed = jnp.where(visible, grad_slots, 0.0).astype(jnp.bfloat16).reshape(-1, D)
    gradients["w_pe"] = (pixels, grad_embed)
    gradients["b_pe"] = column_sums(grad_embed)
    gradients["mask_tok"] = jnp.sum(jnp.where(hidden_mask[..., None], grad_slots, 0.0), (0, 1))
    gradients["cls"] = jnp.sum(jnp.where(is_cls[..., None], grad_slots, 0.0), (0, 1))
    small = jnp.concatenate(
        [jnp.stack([gradients[name] for name in VECTORS]), gradients["b_one"].reshape(-1, D)], 0
    )
    stored_grad = packed_grads(
        span_order, small, [gradients[name] for name, rows, ways in NARROW[1:]], dp
    )
    if own_kernels:
        owned_grad, totals = scatter_all(
            stored_grad, jnp.broadcast_to(part_loss, (8, 128)), 2
        )
        owned_grad = owned_grad.reshape(-1, D)
        total_loss, squares = (totals[0, 0], totals[1, 0])
    else:
        owned_grad = lax.psum_scatter(
            stored_grad.reshape(-1, D), "dp", scatter_dimension=0, tiled=True)
        owned_grad = lax.psum(owned_grad, "seq")
        total_loss = lax.psum(part_loss, ("dp", "seq"))
        squares = lax.psum(jnp.sum(owned_grad * owned_grad), "dp")
    grad_norm = jnp.sqrt(squares)
    clipped = owned_grad * (CLIP / jnp.maximum(grad_norm, CLIP))
    updated_first = BETA_ONE * first_moment + (1.0 - BETA_ONE) * clipped
    updated_second = BETA_TWO * second_moment + (1.0 - BETA_TWO) * clipped * clipped
    steps_done = step_count[0].astype(jnp.float32)
    adam_step = (
        updated_first
        / (1.0 - BETA_ONE**steps_done)
        / (jnp.sqrt(updated_second / (1.0 - BETA_TWO**steps_done)) + ADAM_EPS)
    )
    updated_weights = weights - LEARN * (adam_step + DECAY * weights)
    return (
        total_loss,
        grad_norm,
        updated_weights,
        updated_weights.astype(jnp.bfloat16),
        updated_first,
        updated_second,
    )


def solution(mesh):
    placed = (
        P("dp", "seq", None),
        P("dp", None),
        P("dp"),
        P(),
        P("dp", None),
        P("dp", None),
        P("dp", None),
        P("dp", None),
        P(),
    )
    return jax.shard_map(
        on_device,
        mesh=mesh,
        in_specs=placed,
        out_specs=(P(), P(), P("dp", None), P("dp", None), P("dp", None), P("dp", None)),
        check_vma=False,
    )
```
